8 devices in a mesh: fsdp: 8 (over z, y, x, core).
Axes of the slice: x: 2, y: 2, z: 1, core: 2. Of those that a mesh axis runs over, the one named last changes fastest.
Arguments:
- tok_ids: int32 [8, 4096], P('fsdp')
- tok_labels: int32 [8, 4096], P('fsdp')
- embed: bfloat16 [32128, 768], P('fsdp')
- w_gate: bfloat16 [768, 3072], P('fsdp')
- w_up: bfloat16 [768, 3072], P('fsdp')
- w_down: bfloat16 [3072, 768], P('fsdp')
- gain_mlp: float32 [768], replicated
- gain_final: float32 [768], replicated
Outputs:
- output 1: float32 [], replicated
- output 2: float32 [32128, 768], P('fsdp')
- output 3: float32 [768, 3072], P('fsdp')
- output 4: float32 [768, 3072], P('fsdp')
- output 5: float32 [3072, 768], P('fsdp')
All inputs are finite; a program needn't handle non-finite values.
Results may differ from the reference program's by a relative error of at most 0.00906315.
Values are sent between devices in bfloat16 or wider.
A program may use at most 1 GiB of HBM per device.

```python
import math
import jax
import jax.numpy as jnp
from jax import lax

VOCAB_SIZE = 32128
MODEL_DIM = 768
FFN_DIM = 3072
GLOBAL_BATCH = 8
SEQ_LEN = 4096
NUM_CHUNKS = 8
TOKEN_GROUPS = 8
NORM_EPS = 1e-6
CHUNK_ROWS = VOCAB_SIZE // NUM_CHUNKS
NUM_TOKENS = GLOBAL_BATCH * SEQ_LEN
GROUP_TOKENS = NUM_TOKENS // TOKEN_GROUPS
INV_TOKENS = 1.0 / NUM_TOKENS
EMB_SCALE = math.sqrt(MODEL_DIM)


def setup_inputs(seed: int = 0) -> dict:
    base_key = jax.random.key(seed)
    sub_keys = jax.random.split(base_key, 8)
    tok_ids = jax.random.randint(sub_keys[0], (GLOBAL_BATCH, SEQ_LEN), 0, VOCAB_SIZE, dtype=jnp.int32)
    tok_ids = tok_ids.at[0, 0].set(0).at[GLOBAL_BATCH - 1, SEQ_LEN - 1].set(VOCAB_SIZE - 1)
    tok_labels = jax.random.randint(sub_keys[1], (GLOBAL_BATCH, SEQ_LEN), 0, VOCAB_SIZE, dtype=jnp.int32)
    tok_labels = tok_labels.at[0, 0].set(VOCAB_SIZE - 1).at[GLOBAL_BATCH - 1, SEQ_LEN - 1].set(0)
    embed = (jax.random.normal(sub_keys[2], (VOCAB_SIZE, MODEL_DIM), jnp.float32) * MODEL_DIM ** -0.5).astype(jnp.bfloat16)
    w_gate = (jax.random.normal(sub_keys[3], (MODEL_DIM, FFN_DIM), jnp.float32) * MODEL_DIM ** -0.5).astype(jnp.bfloat16)
    w_up = (jax.random.normal(sub_keys[4], (MODEL_DIM, FFN_DIM), jnp.float32) * MODEL_DIM ** -0.5).astype(jnp.bfloat16)
    w_down = (jax.random.normal(sub_keys[5], (FFN_DIM, MODEL_DIM), jnp.float32) * (2.0 * FFN_DIM ** -0.5)).astype(jnp.bfloat16)
    gain_mlp = jax.random.uniform(sub_keys[6], (MODEL_DIM,), jnp.float32, 0.5, 1.5)
    gain_final = jax.random.uniform(sub_keys[7], (MODEL_DIM,), jnp.float32, 1.0, 2.5)
    return dict(tok_ids=tok_ids, tok_labels=tok_labels, embed=embed, w_gate=w_gate, w_up=w_up, w_down=w_down, gain_mlp=gain_mlp, gain_final=gain_final)


def rms_apply(values, gain_vec):
    inv_rms = lax.rsqrt(jnp.mean(values * values, axis=-1, keepdims=True) + NORM_EPS)
    return (values * inv_rms * gain_vec).astype(jnp.bfloat16), inv_rms


def rms_backward(values, inv_rms, gain_vec, grad_out):
    scaled = grad_out * gain_vec
    return inv_rms * scaled - values * (inv_rms ** 3) * jnp.mean(scaled * values, axis=-1, keepdims=True)


def group_grads(ids_grp, lab_grp, d_emb_acc, embed, w_gate, w_up, w_down, gain_mlp, gain_final):
    x_emb = embed[ids_grp].astype(jnp.float32) * EMB_SCALE
    normed, inv_first = rms_apply(x_emb, gain_mlp)
    gate = jnp.dot(normed, w_gate, preferred_element_type=jnp.float32).astype(jnp.bfloat16)
    up_val = jnp.dot(normed, w_up, preferred_element_type=jnp.float32).astype(jnp.bfloat16)
    gate32 = gate.astype(jnp.float32)
    up32 = up_val.astype(jnp.float32)
    hidden_act = (jax.nn.silu(gate32) * up32).astype(jnp.bfloat16)
    mlp_out = jnp.dot(hidden_act, w_down, preferred_element_type=jnp.float32).astype(jnp.bfloat16)
    hid32 = (x_emb + mlp_out.astype(jnp.float32)).astype(jnp.bfloat16).astype(jnp.float32)
    hid_norm, inv_final = rms_apply(hid32, gain_final)
    emb_chunks = embed.reshape(NUM_CHUNKS, CHUNK_ROWS, MODEL_DIM)
    chunk_index = jnp.arange(NUM_CHUNKS, dtype=jnp.int32)
    col_ids = jnp.arange(CHUNK_ROWS, dtype=jnp.int32)

    def chunk_logits(chunk_emb, chunk_idx):
        logits = jnp.dot(hid_norm, chunk_emb.T, preferred_element_type=jnp.float32)
        label_hit = (lab_grp - chunk_idx * CHUNK_ROWS)[:, None] == col_ids[None, :]
        return logits, label_hit

    def fwd_step(carry, chunk_in):
        run_max, run_sum, lab_logit = carry
        logits, label_hit = chunk_logits(chunk_in[0], chunk_in[1])
        new_max = jnp.maximum(run_max, jnp.max(logits, axis=1))
        run_sum = run_sum * jnp.exp(run_max - new_max) + jnp.sum(jnp.exp(logits - new_max[:, None]), axis=1)
        lab_logit = lab_logit + jnp.sum(jnp.where(label_hit, logits, 0.0), axis=1)
        return (new_max, run_sum, lab_logit), None

    zero_tok = jnp.zeros((GROUP_TOKENS,), jnp.float32)
    start_fwd = (jnp.full((GROUP_TOKENS,), -jnp.inf, jnp.float32), zero_tok, zero_tok)
    (run_max, run_sum, lab_logit), unused_fwd = lax.scan(fwd_step, start_fwd, (emb_chunks, chunk_index))
    log_norm = run_max + jnp.log(run_sum)
    loss_part = jnp.sum(log_norm - lab_logit)

    def bwd_step(carry, chunk_in):
        d_hid, d_rows = carry
        logits, label_hit = chunk_logits(chunk_in[0], chunk_in[1])
        prob_mat = jnp.exp(logits - log_norm[:, None])
        grad_logits = ((prob_mat - label_hit.astype(jnp.float32)) * INV_TOKENS).astype(jnp.bfloat16)
        d_rows = d_rows.at[chunk_in[1]].add(jnp.dot(grad_logits.T, hid_norm, preferred_element_type=jnp.float32))
        d_hid = d_hid + jnp.dot(grad_logits, chunk_in[0], preferred_element_type=jnp.float32)
        return (d_hid, d_rows), None

    start_bwd = (jnp.zeros((GROUP_TOKENS, MODEL_DIM), jnp.float32), d_emb_acc.reshape(NUM_CHUNKS, CHUNK_ROWS, MODEL_DIM))
    (d_hid, d_rows), unused_bwd = lax.scan(bwd_step, start_bwd, (emb_chunks, chunk_index))
    d_hidden = rms_backward(hid32, inv_final, gain_final, d_hid)
    d_mlp = d_hidden.astype(jnp.bfloat16)
    d_down = jnp.dot(hidden_act.T, d_mlp, preferred_element_type=jnp.float32)
    d_act = jnp.dot(d_mlp, w_down.T, preferred_element_type=jnp.float32)
    gate_sig = jax.nn.sigmoid(gate32)
    d_gate_pre = (d_act * up32 * gate_sig * (1.0 + gate32 * (1.0 - gate_sig))).astype(jnp.bfloat16)
    d_up_pre = (d_act * gate32 * gate_sig).astype(jnp.bfloat16)
    d_gate = jnp.dot(normed.T, d_gate_pre, preferred_element_type=jnp.float32)
    d_up = jnp.dot(normed.T, d_up_pre, preferred_element_type=jnp.float32)
    d_normed = jnp.dot(d_gate_pre, w_gate.T, preferred_element_type=jnp.float32) + jnp.dot(d_up_pre, w_up.T, preferred_element_type=jnp.float32)
    d_x = (d_hidden + rms_backward(x_emb, inv_first, gain_mlp, d_normed)).astype(jnp.bfloat16)
    d_emb_new = d_rows.reshape(VOCAB_SIZE, MODEL_DIM).at[ids_grp].add(d_x.astype(jnp.float32) * EMB_SCALE)
    return loss_part, d_emb_new, d_gate, d_up, d_down


def reference(tok_ids, tok_labels, embed, w_gate, w_up, w_down, gain_mlp, gain_final):
    ids_groups = tok_ids.reshape(TOKEN_GROUPS, GROUP_TOKENS)
    lab_groups = tok_labels.reshape(TOKEN_GROUPS, GROUP_TOKENS)

    def group_step(carry, group_in):
        loss_acc, d_emb_acc, gate_acc, up_acc, down_acc = carry
        loss_part, d_emb_acc, d_gate, d_up, d_down = group_grads(group_in[0], group_in[1], d_emb_acc, embed, w_gate, w_up, w_down, gain_mlp, gain_final)
        return (loss_acc + loss_part, d_emb_acc, gate_acc + d_gate, up_acc + d_up, down_acc + d_down), None

    start = (jnp.zeros((), jnp.float32), jnp.zeros((VOCAB_SIZE, MODEL_DIM), jnp.float32), jnp.zeros((MODEL_DIM, FFN_DIM), jnp.float32), jnp.zeros((MODEL_DIM, FFN_DIM), jnp.float32), jnp.zeros((FFN_DIM, MODEL_DIM), jnp.float32))
    totals, unused = lax.scan(group_step, start, (ids_groups, lab_groups))
    return (totals[0] * INV_TOKENS, totals[1], totals[2], totals[3], totals[4])
```

```python
import functools
import math
import jax
import jax.numpy as jnp
from jax import lax
from jax.experimental import pallas as pl
from jax.experimental.pallas import tpu as pltpu
from jax.sharding import PartitionSpec as P

NORM_EPS = 1e-6


def dot_plain(left_mat, right_mat):
    return lax.dot_general(left_mat, right_mat, (((1,), (0,)), ((), ())), preferred_element_type=jnp.float32)


def dot_last(left_mat, right_mat):
    return lax.dot_general(left_mat, right_mat, (((1,), (1,)), ((), ())), preferred_element_type=jnp.float32)


def dot_first(left_mat, right_mat):
    return lax.dot_general(left_mat, right_mat, (((0,), (0,)), ((), ())), preferred_element_type=jnp.float32)


def rms_apply(values, gain_vec):
    inv_rms = lax.rsqrt(jnp.mean(values * values, axis=-1, keepdims=True) + NORM_EPS)
    return (values * inv_rms * gain_vec).astype(jnp.bfloat16), inv_rms


def rms_backward(values, inv_rms, gain_vec, grad_out):
    scaled = grad_out * gain_vec
    return inv_rms * scaled - values * (inv_rms ** 3) * jnp.mean(scaled * values, axis=-1, keepdims=True)


def mlp_forward(x_emb, w_gate, w_up, w_down, gain_mlp, gain_final):
    normed, inv_first = rms_apply(x_emb, gain_mlp)
    gate = dot_plain(normed, w_gate).astype(jnp.bfloat16)
    up_val = dot_plain(normed, w_up).astype(jnp.bfloat16)
    hidden_act = (jax.nn.silu(gate.astype(jnp.float32)) * up_val.astype(jnp.float32)).astype(jnp.bfloat16)
    mlp_out = dot_plain(hidden_act, w_down).astype(jnp.bfloat16)
    hid32 = (x_emb + mlp_out.astype(jnp.float32)).astype(jnp.bfloat16).astype(jnp.float32)
    hid_norm, inv_final = rms_apply(hid32, gain_final)
    return hid_norm, (x_emb, inv_first, normed, gate, up_val, hidden_act, hid32, inv_final)


def mlp_backward(d_hid, saved, w_gate, w_up, w_down, gain_mlp, gain_final):
    x_emb, inv_first, normed, gate, up_val, hidden_act, hid32, inv_final = saved
    d_hidden = rms_backward(hid32, inv_final, gain_final, d_hid)
    d_mlp = d_hidden.astype(jnp.bfloat16)
    d_down = dot_first(hidden_act, d_mlp)
    d_act = dot_last(d_mlp, w_down)
    gate32 = gate.astype(jnp.float32)
    gate_sig = jax.nn.sigmoid(gate32)
    d_gate_pre = (d_act * up_val.astype(jnp.float32) * gate_sig * (1.0 + gate32 * (1.0 - gate_sig))).astype(jnp.bfloat16)
    d_up_pre = (d_act * gate32 * gate_sig).astype(jnp.bfloat16)
    d_gate = dot_first(normed, d_gate_pre)
    d_up = dot_first(normed, d_up_pre)
    d_normed = dot_last(d_gate_pre, w_gate) + dot_last(d_up_pre, w_up)
    d_x = (d_hidden + rms_backward(x_emb, inv_first, gain_mlp, d_normed)).astype(jnp.bfloat16)
    return d_x, d_gate, d_up, d_down


VM = 64 * 1024 * 1024 - 128 * 1024


def nn(a, b):
    return lax.dot_general(a, b, (((1,), (0,)), ((), ())), preferred_element_type=jnp.float32)


def fwd_kernel(emb_ref, hnt_ref, lse_ref, et_ref, max_ref, sum_ref, top_ref, part_ref, *, n_own, n_blk, rows, tail, tok_tile):
    own, blk = pl.program_id(0), pl.program_id(1)
    tok = hnt_ref.shape[1]
    n_tile = tok // tok_tile

    def logits(emb, cols):
        return nn(emb, hnt_ref[:, cols]).reshape(emb.shape[0] // 8, 8, tok_tile)

    def redo(count):
        emb = emb_ref[0, :count, :]

        def tile(i, carry):
            cols = pl.ds(pl.multiple_of(i * tok_tile, tok_tile), tok_tile)
            z = logits(emb, cols)
            old = max_ref[:, cols]
            new = jnp.maximum(old, jnp.max(z, axis=0))
            max_ref[:, cols] = new
            sum_ref[:, cols] = sum_ref[:, cols] * jnp.exp(old - new) + jnp.sum(jnp.exp(z - new[None]), axis=0)
            return carry

        lax.fori_loop(0, n_tile, tile, 0)

    def run(count):
        emb = emb_ref[0, :count, :]
        et_ref[0, :, :count] = emb.T
        for i in range(n_tile):
            cols = slice(i * tok_tile, (i + 1) * tok_tile)
            z = logits(emb, cols)
            shift = max_ref[:, cols]
            top_ref[:, cols] = jnp.max(z, axis=0) - shift
            part_ref[:, cols] = jnp.sum(jnp.exp(z - shift[None]), axis=0)
        grown = jnp.max(top_ref[...]) > 40.0

        @pl.when(grown)
        def _():
            redo(count)

        @pl.when(jnp.logical_not(grown))
        def _():
            sum_ref[...] += part_ref[...]

    @pl.when((own == 0) & (blk == 0))
    def _():
        max_ref[...] = jnp.full(max_ref.shape, -jnp.inf, jnp.float32)
        sum_ref[...] = jnp.zeros(sum_ref.shape, jnp.float32)
        et_ref[0] = emb_ref[0].T
        redo(rows)

    @pl.when((blk < n_blk - 1) & ((own > 0) | (blk > 0)))
    def _():
        run(rows)

    @pl.when(blk == n_blk - 1)
    def _():
        run(tail)

    @pl.when((own == n_own - 1) & (blk == n_blk - 1))
    def _():
        top = jnp.max(max_ref[...], axis=0, keepdims=True)
        total = jnp.sum(sum_ref[...] * jnp.exp(max_ref[...] - top), axis=0, keepdims=True)
        lse_ref[...] = top + jnp.log(total)


def head_fwd(emb3, hnt, rows=512, tok_tile=1024):
    n_own, per, dim = emb3.shape
    tok = hnt.shape[1]
    n_blk = pl.cdiv(per, rows)
    tail = per - (n_blk - 1) * rows
    return pl.pallas_call(
        functools.partial(fwd_kernel, n_own=n_own, n_blk=n_blk, rows=rows, tail=tail, tok_tile=tok_tile),
        grid=(n_own, n_blk),
        in_specs=[pl.BlockSpec((1, rows, dim), lambda o, b: (o, b, 0)),
                  pl.BlockSpec((dim, tok), lambda o, b: (0, 0))],
        out_specs=[pl.BlockSpec((1, tok), lambda o, b: (0, 0)),
                   pl.BlockSpec((1, dim, rows), lambda o, b: (o, 0, b))],
        out_shape=[jax.ShapeDtypeStruct((1, tok), jnp.float32),
                   jax.ShapeDtypeStruct((n_own, dim, per), jnp.bfloat16)],
        scratch_shapes=[pltpu.VMEM((8, tok), jnp.float32)] * 4,
        compiler_params=pltpu.CompilerParams(dimension_semantics=("arbitrary", "arbitrary"), vmem_limit_bytes=VM),
        cost_estimate=pl.CostEstimate(flops=2 * tok * n_own * per * dim, bytes_accessed=4 * n_own * per * dim, transcendentals=tok * n_own * per),
    )(emb3, hnt)


def bwd_kernel(*refs, first, rows, tok_tile, sub, n_own, per, chunk, block, inv_count):
    if first:
        hn_hbm, hnt_hbm, lse_ref, lab_ref, emb_ref, et_ref, de_ref, zy_ref, dhn_hbm = refs[:9]
        dhn_src = None
        rest = refs[9:]
    else:
        hn_hbm, hnt_hbm, lse_ref, lab_ref, emb_ref, et_ref, dhn_src, de_ref, zy_ref, dhn_hbm = refs[:10]
        rest = refs[10:]
    hn_ref, hnt_ref, dhn_ref, hn_sem, hnt_sem, in_sem, out_sem = rest
    own = pl.program_id(0)
    tok, dim = hn_ref.shape
    step = tok_tile * sub
    n_step = tok // step

    def copies(i):
        cols = pl.ds(pl.multiple_of(i * step, step), step)
        out = [pltpu.make_async_copy(hn_hbm.at[cols, :], hn_ref.at[cols, :], hn_sem.at[i]),
               pltpu.make_async_copy(hnt_hbm.at[:, cols], hnt_ref.at[:, cols], hnt_sem.at[i])]
        if not first:
            out.append(pltpu.make_async_copy(dhn_src.at[:, cols], dhn_ref.at[:, cols], in_sem.at[i]))
        return out

    def out_copy(i):
        cols = pl.ds(pl.multiple_of(i * step, step), step)
        return pltpu.make_async_copy(dhn_ref.at[:, cols], dhn_hbm.at[:, cols], out_sem.at[i])

    @pl.when(own == 0)
    def _():
        for i in range(n_step):
            for c in copies(i):
                c.start()
        zy_ref[...] = jnp.zeros(zy_ref.shape, jnp.float32)
        if first:
            dhn_ref[...] = jnp.zeros(dhn_ref.shape, jnp.float32)

    de_ref[...] = jnp.zeros(de_ref.shape, jnp.float32)
    base = own * per + chunk * block
    emb = emb_ref[0, :rows, :]
    emb_t = et_ref[0, :, :rows]

    def tile(i, carry):
        @pl.when(own == 0)
        def _():
            for c in copies(i):
                c.wait()

        row_ids = lax.broadcasted_iota(jnp.int32, (rows, tok_tile), 0)
        work = []
        for s in range(sub):
            cols = pl.ds(pl.multiple_of(i * step + s * tok_tile, tok_tile), tok_tile)
            work.append((cols, nn(emb, hnt_ref[:, cols])))
        grads = []
        for cols, z in work:
            hit = row_ids == (lab_ref[:, cols] - base)
            prob = jnp.exp(z - lse_ref[:, cols])
            grad = (jnp.where(hit, prob - 1.0, prob) * inv_count).astype(jnp.bfloat16)
            zy_ref[:, cols] += jnp.sum(jnp.where(hit, z, 0.0).reshape(rows // 8, 8, tok_tile), axis=0)
            grads.append((cols, grad))
        for cols, grad in grads:
            dhn_ref[:, cols] += nn(emb_t, grad)
        big = grads[0][1] if sub == 1 else jnp.concatenate([g for _, g in grads], axis=1)
        cols = pl.ds(pl.multiple_of(i * step, step), step)
        de_ref[0] += nn(big, hn_ref[cols, :])

        @pl.when(own == n_own - 1)
        def _():
            out_copy(i).start()
        return carry

    lax.fori_loop(0, n_step, tile, 0)

    @pl.when(own == n_own - 1)
    def _():
        for i in range(n_step):
            out_copy(i).wait()


def head_bwd(hn, hnt, lse, lab, emb3, et3, dhn, chunk, block=512, tok_tile=512, sub=2, inv_count=1.0 / 32768):
    n_own, per, dim = emb3.shape
    tok = hn.shape[0]
    rows = min(block, per - chunk * block)
    first = dhn is None
    n_step = tok // (tok_tile * sub)
    anyspec = pl.BlockSpec(memory_space=pl.ANY)
    row = pl.BlockSpec((1, tok), lambda o: (0, 0))
    ins = [hn, hnt, lse, lab, emb3, et3] + ([] if first else [dhn])
    return pl.pallas_call(
        functools.partial(bwd_kernel, first=first, rows=rows, tok_tile=tok_tile, sub=sub, n_own=n_own, per=per, chunk=chunk, block=block, inv_count=inv_count),
        grid=(n_own,),
        in_specs=[anyspec, anyspec, row, row,
                  pl.BlockSpec((1, block, dim), lambda o: (o, chunk, 0)),
                  pl.BlockSpec((1, dim, block), lambda o: (o, 0, chunk))] + ([] if first else [anyspec]),
        out_specs=[pl.BlockSpec((1, rows, dim), lambda o: (o, 0, 0)), pl.BlockSpec((8, tok), lambda o: (0, 0)), anyspec],
        out_shape=[jax.ShapeDtypeStruct((n_own, rows, dim), jnp.float32), jax.ShapeDtypeStruct((8, tok), jnp.float32),
                   jax.ShapeDtypeStruct((dim, tok), jnp.float32)],
        scratch_shapes=[pltpu.VMEM((tok, dim), jnp.bfloat16), pltpu.VMEM((dim, tok), jnp.bfloat16), pltpu.VMEM((dim, tok), jnp.float32)]
        + [pltpu.SemaphoreType.DMA((n_step,))] * 4,
        input_output_aliases={} if first else {6: 2},
        compiler_params=pltpu.CompilerParams(dimension_semantics=("arbitrary",), vmem_limit_bytes=VM),
        cost_estimate=pl.CostEstimate(flops=6 * tok * n_own * rows * dim, bytes_accessed=50 * 1024 * 1024, transcendentals=tok * n_own * rows),
    )(*ins)


def scatter_kernel(meta_ref, live_ref, ids_ref, dx_hbm, base_ref, out_ref, buf_ref, sem, *, rows, toks, scale):
    blk = pl.program_id(0)
    n_live = meta_ref[0]

    def fetch(j, slot):
        start = pl.multiple_of(live_ref[j] * toks, toks)
        return pltpu.make_async_copy(dx_hbm.at[pl.ds(start, toks), :], buf_ref.at[slot], sem.at[slot])

    @pl.when(n_live > 0)
    def _():
        fetch(0, 0).start()

    out_ref[...] = jnp.zeros(out_ref.shape, jnp.float32)
    row_ids = lax.broadcasted_iota(jnp.int32, (rows, toks), 0) + (blk * rows + meta_ref[1])

    def body(j, carry):
        slot = lax.rem(j, 2)

        @pl.when(j + 1 < n_live)
        def _():
            fetch(j + 1, 1 - slot).start()

        fetch(j, slot).wait()
        cols = pl.ds(pl.multiple_of(live_ref[j] * toks, toks), toks)
        hot = jnp.where(row_ids == ids_ref[:, cols], 1.0, 0.0).astype(jnp.bfloat16)
        out_ref[...] += nn(hot, buf_ref[slot])
        return carry

    lax.fori_loop(0, n_live, body, 0)
    out_ref[...] = base_ref[...] + out_ref[...] * scale


def scatter_rows(ids, d_x, base, first_row, scale, rows=1024, toks=256):
    per, dim = base.shape
    n_blk = ids.shape[0] // toks
    live = jnp.any(((ids >= first_row) & (ids < first_row + per)).reshape(n_blk, toks), axis=1)
    order = jnp.argsort(jnp.logical_not(live)).astype(jnp.int32)
    meta = jnp.stack([jnp.sum(live.astype(jnp.int32)), first_row])
    return pl.pallas_call(
        functools.partial(scatter_kernel, rows=rows, toks=toks, scale=scale),
        grid_spec=pltpu.PrefetchScalarGridSpec(
            num_scalar_prefetch=2, grid=(pl.cdiv(per, rows),),
            in_specs=[pl.BlockSpec((1, ids.shape[0]), lambda b, *_: (0, 0)), pl.BlockSpec(memory_space=pl.ANY),
                      pl.BlockSpec((rows, dim), lambda b, *_: (b, 0))],
            out_specs=pl.BlockSpec((rows, dim), lambda b, *_: (b, 0)),
            scratch_shapes=[pltpu.VMEM((2, toks, dim), d_x.dtype), pltpu.SemaphoreType.DMA((2,))]),
        out_shape=jax.ShapeDtypeStruct((per, dim), jnp.float32),
        compiler_params=pltpu.CompilerParams(dimension_semantics=("arbitrary",), vmem_limit_bytes=VM),
        cost_estimate=pl.CostEstimate(flops=2 * per * 8192 * dim, bytes_accessed=8 * per * dim, transcendentals=0),
    )(meta, order, ids.reshape(1, -1), d_x, base)


def solution(mesh):
    group = mesh.shape['fsdp']

    def local_step(ids_blk, lab_blk, emb_shard, gate_shard, up_shard, down_shard, gain_mlp, gain_final):
        me = lax.axis_index('fsdp')
        per, model_dim = emb_shard.shape
        emb_scale = math.sqrt(model_dim)
        ids_flat, lab_flat = lax.sort((ids_blk.reshape(-1), lab_blk.reshape(-1)), num_keys=1)
        n_tok = ids_flat.shape[0]
        inv_count = 1.0 / (n_tok * group)
        embed_full = lax.all_gather(emb_shard, 'fsdp', tiled=True)
        w_gate = lax.all_gather(gate_shard, 'fsdp', tiled=True)
        w_up = lax.all_gather(up_shard, 'fsdp', tiled=True)
        w_down = lax.all_gather(down_shard, 'fsdp', tiled=True)

        ids_all = lax.all_gather(ids_flat, 'fsdp', tiled=True)

        x_emb = jnp.take(embed_full, ids_flat, axis=0, indices_are_sorted=True).astype(jnp.float32) * emb_scale
        hid_norm, saved = mlp_forward(x_emb, w_gate, w_up, w_down, gain_mlp, gain_final)
        hid_t = hid_norm.T
        emb3 = embed_full.reshape(group, per, model_dim)
        log_norm, emb_t = head_fwd(emb3, hid_t)
        labels = lab_flat.reshape(1, -1)
        block = 512
        d_hid_t, lab_logit, d_rows = None, 0.0, []
        for chunk in range(pl.cdiv(per, block)):
            d_emb, lab_part, d_hid_t = head_bwd(hid_norm, hid_t, log_norm, labels, emb3, emb_t, d_hid_t, chunk, block=block, tok_tile=1024, sub=1, inv_count=inv_count)
            d_rows.append(lax.psum_scatter(d_emb, 'fsdp', scatter_dimension=0, tiled=True)[0])
            lab_logit = lab_logit + lab_part
        loss = lax.psum(jnp.sum(log_norm[0] - jnp.sum(lab_logit, axis=0)), 'fsdp') * inv_count

        d_x, d_gate, d_up, d_down = mlp_backward(d_hid_t.T, saved, w_gate, w_up, w_down, gain_mlp, gain_final)
        d_gate = lax.psum_scatter(d_gate, 'fsdp', scatter_dimension=0, tiled=True)
        d_up = lax.psum_scatter(d_up, 'fsdp', scatter_dimension=0, tiled=True)
        d_down = lax.psum_scatter(d_down, 'fsdp', scatter_dimension=0, tiled=True)
        d_x_all = lax.all_gather(d_x, 'fsdp', tiled=True)
        d_embed = scatter_rows(ids_all, d_x_all, jnp.concatenate(d_rows, axis=0), me * per, emb_scale)
        return loss, d_embed, d_gate, d_up, d_down

    shard_spec = P('fsdp', None)
    return jax.shard_map(local_step, mesh=mesh, in_specs=(shard_spec, shard_spec, shard_spec, shard_spec, shard_spec, shard_spec, P(), P()), out_specs=(P(), shard_spec, shard_spec, shard_spec, shard_spec), check_vma=False)
```

```python
import functools
import math
import jax
import jax.numpy as jnp
from jax import lax
from jax.experimental import pallas as pl
from jax.experimental.pallas import tpu as pltpu
from jax.sharding import PartitionSpec as P

NORM_EPS = 1e-6


def dot_plain(left_mat, right_mat):
    return lax.dot_general(left_mat, right_mat, (((1,), (0,)), ((), ())), preferred_element_type=jnp.float32)


def dot_last(left_mat, right_mat):
    return lax.dot_general(left_mat, right_mat, (((1,), (1,)), ((), ())), preferred_element_type=jnp.float32)


def dot_first(left_mat, right_mat):
    return lax.dot_general(left_mat, right_mat, (((0,), (0,)), ((), ())), preferred_element_type=jnp.float32)


def rms_apply(values, gain_vec):
    inv_rms = lax.rsqrt(jnp.mean(values * values, axis=-1, keepdims=True) + NORM_EPS)
    return (values * inv_rms * gain_vec).astype(jnp.bfloat16), inv_rms


def rms_backward(values, inv_rms, gain_vec, grad_out):
    scaled = grad_out * gain_vec
    return inv_rms * scaled - values * (inv_rms ** 3) * jnp.mean(scaled * values, axis=-1, keepdims=True)


def mlp_forward(x_emb, w_gate, w_up, w_down, gain_mlp, gain_final):
    normed, inv_first = rms_apply(x_emb, gain_mlp)
    gate = dot_plain(normed, w_gate).astype(jnp.bfloat16)
    up_val = dot_plain(normed, w_up).astype(jnp.bfloat16)
    hidden_act = (jax.nn.silu(gate.astype(jnp.float32)) * up_val.astype(jnp.float32)).astype(jnp.bfloat16)
    mlp_out = dot_plain(hidden_act, w_down).astype(jnp.bfloat16)
    hid32 = (x_emb + mlp_out.astype(jnp.float32)).astype(jnp.bfloat16).astype(jnp.float32)
    hid_norm, inv_final = rms_apply(hid32, gain_final)
    return hid_norm, (x_emb, inv_first, normed, gate, up_val, hidden_act, hid32, inv_final)


def mlp_backward(d_hid, saved, w_gate, w_up, w_down, gain_mlp, gain_final):
    x_emb, inv_first, normed, gate, up_val, hidden_act, hid32, inv_final = saved
    d_hidden = rms_backward(hid32, inv_final, gain_final, d_hid)
    d_mlp = d_hidden.astype(jnp.bfloat16)
    d_down = dot_first(hidden_act, d_mlp)
    d_act = dot_last(d_mlp, w_down)
    gate32 = gate.astype(jnp.float32)
    gate_sig = jax.nn.sigmoid(gate32)
    d_gate_pre = (d_act * up_val.astype(jnp.float32) * gate_sig * (1.0 + gate32 * (1.0 - gate_sig))).astype(jnp.bfloat16)
    d_up_pre = (d_act * gate32 * gate_sig).astype(jnp.bfloat16)
    d_gate = dot_first(normed, d_gate_pre)
    d_up = dot_first(normed, d_up_pre)
    d_normed = dot_last(d_gate_pre, w_gate) + dot_last(d_up_pre, w_up)
    d_x = (d_hidden + rms_backward(x_emb, inv_first, gain_mlp, d_normed)).astype(jnp.bfloat16)
    return d_x, d_gate, d_up, d_down


VM = 64 * 1024 * 1024 - 128 * 1024


def nn(a, b):
    return lax.dot_general(a, b, (((1,), (0,)), ((), ())), preferred_element_type=jnp.float32)


def fwd_kernel(emb_ref, hnt_ref, lse_ref, et_ref, max_ref, sum_ref, top_ref, part_ref, *, n_own, n_blk, rows, tail, tok_tile):
    own, blk = pl.program_id(0), pl.program_id(1)
    tok = hnt_ref.shape[1]
    n_tile = tok // tok_tile

    def logits(emb, cols):
        return nn(emb, hnt_ref[:, cols]).reshape(emb.shape[0] // 8, 8, tok_tile)

    def redo(count):
        emb = emb_ref[0, :count, :]

        def tile(i, carry):
            cols = pl.ds(pl.multiple_of(i * tok_tile, tok_tile), tok_tile)
            z = logits(emb, cols)
            old = max_ref[:, cols]
            new = jnp.maximum(old, jnp.max(z, axis=0))
            max_ref[:, cols] = new
            sum_ref[:, cols] = sum_ref[:, cols] * jnp.exp(old - new) + jnp.sum(jnp.exp(z - new[None]), axis=0)
            return carry

        lax.fori_loop(0, n_tile, tile, 0)

    def run(count):
        emb = emb_ref[0, :count, :]
        et_ref[0, :, :count] = emb.T
        for i in range(n_tile):
            cols = slice(i * tok_tile, (i + 1) * tok_tile)
            z = logits(emb, cols)
            shift = max_ref[:, cols]
            top_ref[:, cols] = jnp.max(z, axis=0) - shift
            part_ref[:, cols] = jnp.sum(jnp.exp(z - shift[None]), axis=0)
        grown = jnp.max(top_ref[...]) > 40.0

        @pl.when(grown)
        def _():
            redo(count)

        @pl.when(jnp.logical_not(grown))
        def _():
            sum_ref[...] += part_ref[...]

    @pl.when((own == 0) & (blk == 0))
    def _():
        max_ref[...] = jnp.full(max_ref.shape, -jnp.inf, jnp.float32)
        sum_ref[...] = jnp.zeros(sum_ref.shape, jnp.float32)
        et_ref[0] = emb_ref[0].T
        redo(rows)

    @pl.when((blk < n_blk - 1) & ((own > 0) | (blk > 0)))
    def _():
        run(rows)

    @pl.when(blk == n_blk - 1)
    def _():
        run(tail)

    @pl.when((own == n_own - 1) & (blk == n_blk - 1))
    def _():
        top = jnp.max(max_ref[...], axis=0, keepdims=True)
        total = jnp.sum(sum_ref[...] * jnp.exp(max_ref[...] - top), axis=0, keepdims=True)
        lse_ref[...] = top + jnp.log(total)


def head_fwd(emb3, hnt, rows=512, tok_tile=1024):
    n_own, per, dim = emb3.shape
    tok = hnt.shape[1]
    n_blk = pl.cdiv(per, rows)
    tail = per - (n_blk - 1) * rows
    return pl.pallas_call(
        functools.partial(fwd_kernel, n_own=n_own, n_blk=n_blk, rows=rows, tail=tail, tok_tile=tok_tile),
        grid=(n_own, n_blk),
        in_specs=[pl.BlockSpec((1, rows, dim), lambda o, b: (o, b, 0)),
                  pl.BlockSpec((dim, tok), lambda o, b: (0, 0))],
        out_specs=[pl.BlockSpec((1, tok), lambda o, b: (0, 0)),
                   pl.BlockSpec((1, dim, rows), lambda o, b: (o, 0, b))],
        out_shape=[jax.ShapeDtypeStruct((1, tok), jnp.float32),
                   jax.ShapeDtypeStruct((n_own, dim, per), jnp.bfloat16)],
        scratch_shapes=[pltpu.VMEM((8, tok), jnp.float32)] * 4,
        compiler_params=pltpu.CompilerParams(dimension_semantics=("arbitrary", "arbitrary"), vmem_limit_bytes=VM),
        cost_estimate=pl.CostEstimate(flops=2 * tok * n_own * per * dim, bytes_accessed=4 * n_own * per * dim, transcendentals=tok * n_own * per),
    )(emb3, hnt)


def bwd_kernel(*refs, first, rows, tok_tile, sub, n_own, per, chunk, block, inv_count):
    if first:
        hn_hbm, hnt_hbm, lse_ref, lab_ref, emb_ref, et_ref, de_ref, zy_ref, dhn_hbm = refs[:9]
        dhn_src = None
        rest = refs[9:]
    else:
        hn_hbm, hnt_hbm, lse_ref, lab_ref, emb_ref, et_ref, dhn_src, de_ref, zy_ref, dhn_hbm = refs[:10]
        rest = refs[10:]
    hn_ref, hnt_ref, dhn_ref, hn_sem, hnt_sem, in_sem, out_sem = rest
    own = pl.program_id(0)
    tok, dim = hn_ref.shape
    step = tok_tile * sub
    n_step = tok // step

    def copies(i):
        cols = pl.ds(pl.multiple_of(i * step, step), step)
        out = [pltpu.make_async_copy(hn_hbm.at[cols, :], hn_ref.at[cols, :], hn_sem.at[i]),
               pltpu.make_async_copy(hnt_hbm.at[:, cols], hnt_ref.at[:, cols], hnt_sem.at[i])]
        if not first:
            out.append(pltpu.make_async_copy(dhn_src.at[:, cols], dhn_ref.at[:, cols], in_sem.at[i]))
        return out

    def out_copy(i):
        cols = pl.ds(pl.multiple_of(i * step, step), step)
        return pltpu.make_async_copy(dhn_ref.at[:, cols], dhn_hbm.at[:, cols], out_sem.at[i])

    @pl.when(own == 0)
    def _():
        for i in range(n_step):
            for c in copies(i):
                c.start()
        zy_ref[...] = jnp.zeros(zy_ref.shape, jnp.float32)
        if first:
            dhn_ref[...] = jnp.zeros(dhn_ref.shape, jnp.float32)

    de_ref[...] = jnp.zeros(de_ref.shape, jnp.float32)
    base = own * per + chunk * block
    emb = emb_ref[0, :rows, :]
    emb_t = et_ref[0, :, :rows]

    def tile(i, carry):
        @pl.when(own == 0)
        def _():
            for c in copies(i):
                c.wait()

        row_ids = lax.broadcasted_iota(jnp.int32, (rows, tok_tile), 0)
        work = []
        for s in range(sub):
            cols = pl.ds(pl.multiple_of(i * step + s * tok_tile, tok_tile), tok_tile)
            work.append((cols, nn(emb, hnt_ref[:, cols])))
        grads = []
        for cols, z in work:
            hit = row_ids == (lab_ref[:, cols] - base)
            prob = jnp.exp(z - lse_ref[:, cols])
            grad = (jnp.where(hit, prob - 1.0, prob) * inv_count).astype(jnp.bfloat16)
            zy_ref[:, cols] += jnp.sum(jnp.where(hit, z, 0.0).reshape(rows // 8, 8, tok_tile), axis=0)
            grads.append((cols, grad))
        for cols, grad in grads:
            dhn_ref[:, cols] += nn(emb_t, grad)
        big = grads[0][1] if sub == 1 else jnp.concatenate([g for _, g in grads], axis=1)
        cols = pl.ds(pl.multiple_of(i * step, step), step)
        de_ref[0] += nn(big, hn_ref[cols, :])

        @pl.when(own == n_own - 1)
        def _():
            out_copy(i).start()
        return carry

    lax.fori_loop(0, n_step, tile, 0)

    @pl.when(own == n_own - 1)
    def _():
        for i in range(n_step):
            out_copy(i).wait()


def head_bwd(hn, hnt, lse, lab, emb3, et3, dhn, chunk, block=512, tok_tile=512, sub=2, inv_count=1.0 / 32768):
    n_own, per, dim = emb3.shape
    tok = hn.shape[0]
    rows = min(block, per - chunk * block)
    first = dhn is None
    n_step = tok // (tok_tile * sub)
    anyspec = pl.BlockSpec(memory_space=pl.ANY)
    row = pl.BlockSpec((1, tok), lambda o: (0, 0))
    ins = [hn, hnt, lse, lab, emb3, et3] + ([] if first else [dhn])
    return pl.pallas_call(
        functools.partial(bwd_kernel, first=first, rows=rows, tok_tile=tok_tile, sub=sub, n_own=n_own, per=per, chunk=chunk, block=block, inv_count=inv_count),
        grid=(n_own,),
        in_specs=[anyspec, anyspec, row, row,
                  pl.BlockSpec((1, block, dim), lambda o: (o, chunk, 0)),
                  pl.BlockSpec((1, dim, block), lambda o: (o, 0, chunk))] + ([] if first else [anyspec]),
        out_specs=[pl.BlockSpec((1, rows, dim), lambda o: (o, 0, 0)), pl.BlockSpec((8, tok), lambda o: (0, 0)), anyspec],
        out_shape=[jax.ShapeDtypeStruct((n_own, rows, dim), jnp.float32), jax.ShapeDtypeStruct((8, tok), jnp.float32),
                   jax.ShapeDtypeStruct((dim, tok), jnp.float32)],
        scratch_shapes=[pltpu.VMEM((tok, dim), jnp.bfloat16), pltpu.VMEM((dim, tok), jnp.bfloat16), pltpu.VMEM((dim, tok), jnp.float32)]
        + [pltpu.SemaphoreType.DMA((n_step,))] * 4,
        input_output_aliases={} if first else {6: 2},
        compiler_params=pltpu.CompilerParams(dimension_semantics=("arbitrary",), vmem_limit_bytes=VM),
        cost_estimate=pl.CostEstimate(flops=6 * tok * n_own * rows * dim, bytes_accessed=50 * 1024 * 1024, transcendentals=tok * n_own * rows),
    )(*ins)


def scatter_kernel(meta_ref, live_ref, ids_ref, dx_hbm, base_ref, out_ref, buf_ref, sem, *, rows, toks, scale):
    blk = pl.program_id(0)
    n_live = meta_ref[0]

    def fetch(j, slot):
        start = pl.multiple_of(live_ref[j] * toks, toks)
        return pltpu.make_async_copy(dx_hbm.at[pl.ds(start, toks), :], buf_ref.at[slot], sem.at[slot])

    @pl.when(n_live > 0)
    def _():
        fetch(0, 0).start()

    out_ref[...] = jnp.zeros(out_ref.shape, jnp.float32)
    row_ids = lax.broadcasted_iota(jnp.int32, (rows, toks), 0) + (blk * rows + meta_ref[1])

    def body(j, carry):
        slot = lax.rem(j, 2)

        @pl.when(j + 1 < n_live)
        def _():
            fetch(j + 1, 1 - slot).start()

        fetch(j, slot).wait()
        cols = pl.ds(pl.multiple_of(live_ref[j] * toks, toks), toks)
        hot = jnp.where(row_ids == ids_ref[:, cols], 1.0, 0.0).astype(jnp.bfloat16)
        out_ref[...] += nn(hot, buf_ref[slot])
        return carry

    lax.fori_loop(0, n_live, body, 0)
    out_ref[...] = base_ref[...] + out_ref[...] * scale


def scatter_rows(ids, d_x, base, first_row, scale, rows=1024, toks=640):
    per, dim = base.shape
    n_blk = ids.shape[0] // toks
    live = jnp.any(((ids >= first_row) & (ids < first_row + per)).reshape(n_blk, toks), axis=1)
    order = jnp.argsort(jnp.logical_not(live)).astype(jnp.int32)
    meta = jnp.stack([jnp.sum(live.astype(jnp.int32)), first_row])
    return pl.pallas_call(
        functools.partial(scatter_kernel, rows=rows, toks=toks, scale=scale),
        grid_spec=pltpu.PrefetchScalarGridSpec(
            num_scalar_prefetch=2, grid=(pl.cdiv(per, rows),),
            in_specs=[pl.BlockSpec((1, ids.shape[0]), lambda b, *_: (0, 0)), pl.BlockSpec(memory_space=pl.ANY),
                      pl.BlockSpec((rows, dim), lambda b, *_: (b, 0))],
            out_specs=pl.BlockSpec((rows, dim), lambda b, *_: (b, 0)),
            scratch_shapes=[pltpu.VMEM((2, toks, dim), d_x.dtype), pltpu.SemaphoreType.DMA((2,))]),
        out_shape=jax.ShapeDtypeStruct((per, dim), jnp.float32),
        compiler_params=pltpu.CompilerParams(dimension_semantics=("arbitrary",), vmem_limit_bytes=VM),
        cost_estimate=pl.CostEstimate(flops=2 * per * 8192 * dim, bytes_accessed=8 * per * dim, transcendentals=0),
    )(meta, order, ids.reshape(1, -1), d_x, base)


def exchange_plan(ids_all, group, per):
    owners = jnp.arange(group, dtype=jnp.int32)
    counts = jnp.sum((ids_all[:, None, :] // per == owners[None, :, None]).astype(jnp.int32), axis=2)
    return counts, jnp.cumsum(counts, axis=1) - counts


def solution(mesh):
    group = mesh.shape['fsdp']

    def local_step(ids_blk, lab_blk, emb_shard, gate_shard, up_shard, down_shard, gain_mlp, gain_final):
        me = lax.axis_index('fsdp')
        per, model_dim = emb_shard.shape
        emb_scale = math.sqrt(model_dim)
        ids_flat, lab_flat = lax.sort((ids_blk.reshape(-1), lab_blk.reshape(-1)), num_keys=1)
        n_tok = ids_flat.shape[0]
        inv_count = 1.0 / (n_tok * group)
        embed_full = lax.all_gather(emb_shard, 'fsdp', tiled=True)
        w_gate = lax.all_gather(gate_shard, 'fsdp', tiled=True)
        w_up = lax.all_gather(up_shard, 'fsdp', tiled=True)
        w_down = lax.all_gather(down_shard, 'fsdp', tiled=True)

        ids_all = lax.all_gather(ids_flat, 'fsdp')
        counts, starts = exchange_plan(ids_all, group, per)
        cap = -(-n_tok * 5 // (group * 4 * 128)) * 128
        rounds = (jnp.max(counts) + cap - 1) // cap
        pad_ids = jnp.pad(ids_all, ((0, 0), (0, cap)), constant_values=-1)

        x_emb = jnp.take(embed_full, ids_flat, axis=0, indices_are_sorted=True).astype(jnp.float32) * emb_scale
        hid_norm, saved = mlp_forward(x_emb, w_gate, w_up, w_down, gain_mlp, gain_final)
        hid_t = hid_norm.T
        emb3 = embed_full.reshape(group, per, model_dim)
        log_norm, emb_t = head_fwd(emb3, hid_t, rows=1024)
        labels = lab_flat.reshape(1, -1)
        block = 768
        d_hid_t, lab_logit, d_rows = None, 0.0, []
        for chunk in range(pl.cdiv(per, block)):
            d_emb, lab_part, d_hid_t = head_bwd(hid_norm, hid_t, log_norm, labels, emb3, emb_t, d_hid_t, chunk, block=block, tok_tile=1024, sub=1, inv_count=inv_count)
            d_rows.append(lax.psum_scatter(d_emb, 'fsdp', scatter_dimension=0, tiled=True)[0])
            lab_logit = lab_logit + lab_part
        loss = lax.psum(jnp.sum(log_norm[0] - jnp.sum(lab_logit, axis=0)), 'fsdp') * inv_count

        d_x, d_gate, d_up, d_down = mlp_backward(d_hid_t.T, saved, w_gate, w_up, w_down, gain_mlp, gain_final)
        d_gate = lax.psum_scatter(d_gate, 'fsdp', scatter_dimension=0, tiled=True)
        d_up = lax.psum_scatter(d_up, 'fsdp', scatter_dimension=0, tiled=True)
        d_down = lax.psum_scatter(d_down, 'fsdp', scatter_dimension=0, tiled=True)
        pad_d_x = jnp.pad(d_x, ((0, cap), (0, 0)))

        def exchange_round(turn, d_embed):
            send = jnp.concatenate([lax.dynamic_slice(pad_d_x, (starts[me, own] + turn * cap, 0), (cap, model_dim)) for own in range(group)], axis=0)
            ids = jnp.concatenate([lax.dynamic_slice(pad_ids, (src, starts[src, me] + turn * cap), (1, cap)) for src in range(group)], axis=1)
            got = lax.all_to_all(send, 'fsdp', 0, 0, tiled=True)
            return scatter_rows(ids.reshape(-1), got, d_embed, me * per, emb_scale, toks=cap)

        d_embed = exchange_round(0, jnp.concatenate(d_rows, axis=0))
        d_embed = lax.fori_loop(1, rounds, exchange_round, d_embed)
        return loss, d_embed, d_gate, d_up, d_down

    shard_spec = P('fsdp', None)
    return jax.shard_map(local_step, mesh=mesh, in_specs=(shard_spec, shard_spec, shard_spec, shard_spec, shard_spec, shard_spec, P(), P()), out_specs=(P(), shard_spec, shard_spec, shard_spec, shard_spec), check_vma=False)
```
